32 devices in a mesh: seq: 8 (over z, x), head: 4 (over y, core).
Axes of the slice: x: 2, y: 2, z: 4, core: 2. Of those that a mesh axis runs over, the one named last changes fastest.
Arguments:
- queries: bfloat16 [2, 512, 8192], P(None, 'seq', 'head'), may hold values from -256 to 256
- keys: bfloat16 [2, 2048, 1024], P(None, 'seq', 'head'), may hold values from -12 to 12
- lengths: int32 [2], replicated, may hold values from 768 to 2048, as said below
- starts: int32 [2], replicated, may hold values from 0 to 256, as said below
Outputs:
- key_scores: float32 [2, 8, 2048], P(None, 'head', 'seq')
- token_scores: float32 [2, 2048], P(None, 'seq')
The draws below stay inside these ranges and needn't reach their ends.
Inputs may be any that keep to these rules, and one draw needn't show every extreme that they name: `lengths`: every length is a multiple of 128 and at least 768; in every draw one request has length 2048. `starts`: each start is at most its request's length minus 512 minus 128; in every draw one start equals 256.
All inputs are finite; a program needn't handle non-finite values.
Results may differ from the reference program's by a relative error of at most 0.0003.
Values may be sent and summed in bfloat16 or wider, within the bound.
A program may use at most 64 MiB of HBM per device.

```python
import jax
import jax.numpy as jnp
from jax import lax

H = 64
KVH = 8
D = 128
QLEN = 512
REQS = 2
CTX = 2048


def integer_draws(key):
    key_len, key_full, key_start = jax.random.split(jax.random.fold_in(key, 7), 3)
    lowest_block = (QLEN + 256 + 127) // 128
    highest_block = CTX // 128
    blocks = jax.random.randint(key_len, (REQS,), lowest_block, max(highest_block, lowest_block + 1))
    full_request = jax.random.randint(key_full, (), 0, REQS)
    is_full = jnp.arange(REQS) == full_request
    blocks = jnp.where(is_full, highest_block, blocks)
    lengths = (blocks * 128).astype(jnp.int32)
    upper = jnp.minimum(CTX // 8, lengths - QLEN - 128)
    starts = jax.random.randint(key_start, (REQS,), 0, upper + 1)
    starts = jnp.where(is_full, CTX // 8, starts).astype(jnp.int32)
    return (lengths, starts)


def key_entries(key):
    entries = jax.random.normal(jax.random.fold_in(key, 21), (REQS, CTX, KVH, D), jnp.float32)
    entries = jnp.clip(entries, -6.0, 6.0)
    return entries


def draw_lengths(key, part):
    return integer_draws(key)[0]


def draw_starts(key, part):
    return integer_draws(key)[1]


def draw_keys(key, part):
    return key_entries(key).reshape(REQS, CTX, KVH * D).astype(jnp.bfloat16)


def draw_queries(key, part):
    entries = jax.random.normal(jax.random.fold_in(key, 31), (REQS, QLEN, H, D), jnp.float32)
    entries = jnp.clip(entries, -6.0, 6.0)
    return entries.reshape(REQS, QLEN, H * D).astype(jnp.bfloat16)


def setup_inputs(seed: int = 0) -> dict:
    splits = jax.random.split(jax.random.key(seed), 5)
    queries = draw_queries(jax.random.fold_in(splits[4], 71), 0)
    keys = draw_keys(jax.random.fold_in(splits[4], 71), 0)
    lengths = draw_lengths(jax.random.fold_in(splits[4], 71), 0)
    starts = draw_starts(jax.random.fold_in(splits[4], 71), 0)
    return {"queries": queries, "keys": keys, "lengths": lengths, "starts": starts}


MASK_FILL = -1e30


def reference(queries, keys, lengths, starts):
    group_size = H // KVH
    score_scale = D ** -0.5
    query_all = queries.reshape(REQS, QLEN, KVH, group_size, D)
    key_all = keys.reshape(REQS, CTX, KVH, D)
    key_pos = jnp.arange(CTX, dtype=jnp.int32)

    def column_sums_of(item_index):
        request_id = item_index // KVH
        head_id = item_index % KVH
        query_block = lax.dynamic_index_in_dim(query_all, request_id, 0, keepdims=False)
        query_block = lax.dynamic_index_in_dim(query_block, head_id, 1, keepdims=False)
        key_block = lax.dynamic_index_in_dim(key_all, request_id, 0, keepdims=False)
        key_block = lax.dynamic_index_in_dim(key_block, head_id, 1, keepdims=False)
        scores = jnp.einsum("thd,kd->htk", query_block.astype(jnp.float32), key_block.astype(jnp.float32),
                            precision=lax.Precision.HIGHEST) * score_scale
        length = lengths[request_id]
        start = starts[request_id]
        query_pos = length - QLEN + jnp.arange(QLEN, dtype=jnp.int32)
        allowed = (key_pos[None, :] <= query_pos[:, None]) & (key_pos[None, :] >= start)
        masked = jnp.where(allowed[None], scores, MASK_FILL)
        row_max = jnp.max(masked, axis=2, keepdims=True)
        expos = jnp.where(allowed[None], jnp.exp(masked - row_max), 0.0)
        row_sum = jnp.sum(expos, axis=2, keepdims=True)
        probs = expos / row_sum
        return jnp.sum(probs, axis=(0, 1))

    columns = lax.map(column_sums_of, jnp.arange(REQS * KVH, dtype=jnp.int32))
    key_scores = columns.reshape(REQS, KVH, CTX)
    token_scores = jnp.sum(key_scores, axis=1)
    return key_scores, token_scores
```

```python
import functools

import jax
import jax.numpy as jnp
from jax import lax
from jax.experimental import pallas as pl
from jax.experimental.pallas import tpu as pltpu
from jax.sharding import PartitionSpec as P

KVH = 8
D = 128
QLEN = 512
MASK_FILL = -1e30
MASK_FLOOR = -5e29
LOG2E = 1.4426950408889634
MESH = pl.DeviceIdType.MESH


def kernel(
    n_seq, n_head, starts_ref, lengths_ref, q_hbm, k_hbm, key_out, tok_out,
    qs, ks, es, ms, ls, ws, stat, stat_in, cols, cols_in, tok, tok_in,
    q_sem, k_sem, q_send, q_recv, up_send, down_send, k_recv,
    stat_send, stat_recv, col_send, col_recv, tok_send, tok_recv,
):
    requests, tokens, width = q_hbm.shape
    block = k_hbm.shape[1]
    groups = k_hbm.shape[2] // D
    heads = width // (groups * D)
    rows = heads * tokens
    chain = n_seq // 2
    tile = min(256, rows)
    scale = (D ** -0.5) * LOG2E
    me = lax.axis_index("seq")
    head = lax.axis_index("head")
    pair = lax.rem(me, 2)
    spot = me // 2

    def at(seq, hd=None):
        return {"seq": seq, "head": head if hd is None else hd}

    def chain_dev(i):
        return at(i * 2 + pair)

    peer = at(me + 1 - 2 * pair)

    for b in range(requests):
        pltpu.make_async_copy(k_hbm.at[b], ks.at[spot, b], k_sem.at[b]).start()
        for g in range(groups):
            for h in range(heads):
                pltpu.make_async_copy(
                    q_hbm.at[b, :, pl.ds((g * heads + h) * D, D)], qs.at[pair, b, g, h], q_sem.at[b]
                ).start()

    barrier = pltpu.get_barrier_semaphore()
    for d in range(1, chain):
        pl.semaphore_signal(barrier, inc=1, device_id=chain_dev(lax.rem(spot + d, chain)), device_id_type=MESH)
    pl.semaphore_signal(barrier, inc=1, device_id=peer, device_id_type=MESH)
    for d in range(1, n_head):
        pl.semaphore_signal(
            barrier, inc=1, device_id=at(me, lax.rem(head + d, n_head)), device_id_type=MESH
        )
    pl.semaphore_wait(barrier, chain - 1 + 1 + n_head - 1)

    def key_copy(i, b, upward):
        sems = up_send if upward else down_send
        return pltpu.make_async_remote_copy(
            src_ref=ks.at[i, b], dst_ref=ks.at[i, b], send_sem=sems.at[i, b], recv_sem=k_recv.at[i, b],
            device_id=chain_dev(spot + 1 if upward else spot - 1), device_id_type=MESH,
        )

    def send_key(i, b, upward):
        @pl.when((spot < chain - 1) if upward else (spot > 0))
        def _():
            key_copy(i, b, upward).start()

    def query_copy(b):
        return pltpu.make_async_remote_copy(
            src_ref=qs.at[pair, b], dst_ref=qs.at[pair, b], send_sem=q_send.at[b], recv_sem=q_recv.at[b],
            device_id=peer, device_id_type=MESH,
        )

    for b in range(requests):
        pltpu.make_async_copy(k_hbm.at[b], ks.at[spot, b], k_sem.at[b]).wait()
        send_key(spot, b, True)
        send_key(spot, b, False)
    for b in range(requests):
        pltpu.make_async_copy(qs.at[pair, b], qs.at[pair, b], q_sem.at[b]).wait()
        query_copy(b).start()

    def work(i, b, first, count):
        start = starts_ref[b]
        length = lengths_ref[b]
        keypos = (i * 2 + pair) * block + lax.broadcasted_iota(jnp.int32, (block, tile), 0)
        lane_token = lax.rem(lax.broadcasted_iota(jnp.int32, (1, tile), 1), tokens)

        def step(u, carry):
            slot = lax.rem(first + u // groups, 2)
            g = lax.rem(u, groups)
            where = (b * 2 + slot) * groups + g
            k = ks[i, b, :, pl.ds(pl.multiple_of(g * D, D), D)]
            q = qs[slot, b, g].reshape(rows, D)
            pos = length - QLEN + (spot * 2 + slot) * tokens + lane_token
            for r in range(rows // tile):
                s = lax.dot_general(
                    k, q[r * tile:(r + 1) * tile], (((1,), (1,)), ((), ())),
                    preferred_element_type=jnp.float32,
                )
                allowed = (keypos <= pos) & (keypos >= start)
                s = jnp.where(allowed, s, MASK_FILL)
                top = jnp.maximum(jnp.max(s, axis=0, keepdims=True), MASK_FLOOR)
                e = jnp.exp2((s - top) * scale)
                es[i, b, slot, g, :, r * tile:(r + 1) * tile] = e
                ms[i, pl.ds(where, 1), r * tile:(r + 1) * tile] = top
                ls[i, pl.ds(where, 1), r * tile:(r + 1) * tile] = jnp.sum(e, axis=0, keepdims=True)
            return carry

        lax.fori_loop(0, count * groups, step, 0)

    own, other = pair, 1 - pair

    for b in range(requests):
        work(spot, b, own, 1)

    def receive(s, b, count):
        @pl.when(spot - s >= 0)
        def _():
            key_copy(spot - s, b, True).wait_recv()
            send_key(spot - s, b, True)

        @pl.when(spot + s < chain)
        def _():
            key_copy(spot + s, b, False).wait_recv()
            send_key(spot + s, b, False)

        def side(v, carry):
            i = spot - s + v * 2 * s

            @pl.when((i >= 0) & (i < chain))
            def _():
                work(i, b, own, count)

            return carry

        lax.fori_loop(0, 2, side, 0)

    def catch_up(b, reach):
        query_copy(b).wait_recv()

        def one(i, carry):
            work(i, b, other, 1)
            return carry

        lax.fori_loop(jnp.maximum(spot - reach, 0), jnp.minimum(spot + reach, chain - 1) + 1, one, 0)

    last = chain - 1
    for b in range(requests):
        receive(1, b, 1) if last >= 1 else None
    early = min(1, last)
    for b in range(requests - 1):
        catch_up(b, early)

    def middle(s, carry):
        for b in range(requests - 1):
            receive(s, b, 2)
        receive(s, requests - 1, 1)
        return carry

    if last > 1:
        lax.fori_loop(2, last, middle, 0)
        for b in range(requests - 1):
            receive(last, b, 2)
        catch_up(requests - 1, last - 1)
        receive(last, requests - 1, 2)
    else:
        catch_up(requests - 1, last)

    top = ms[0]
    for i in range(1, chain):
        top = jnp.maximum(top, ms[i])
    total = ls[0] * jnp.exp2((ms[0] - top) * scale)
    for i in range(1, chain):
        total += ls[i] * jnp.exp2((ms[i] - top) * scale)
    stat[0] = top
    stat[1] = total
    stat_copy = pltpu.make_async_remote_copy(
        src_ref=stat, dst_ref=stat_in, send_sem=stat_send, recv_sem=stat_recv,
        device_id=peer, device_id_type=MESH,
    )
    stat_copy.start()
    stat_copy.wait()
    full_top = jnp.maximum(stat[0], stat_in[0])
    full = stat[1] * jnp.exp2((stat[0] - full_top) * scale) + stat_in[1] * jnp.exp2(
        (stat_in[0] - full_top) * scale
    )
    inverse = 1.0 / full
    for i in range(chain):
        weight = jnp.exp2((ms[i] - full_top) * scale) * inverse
        for u in range(weight.shape[0]):
            ws[i, u] = weight[u:u + 1]

    ones = jnp.ones((8, 128 if rows >= 128 else rows), jnp.float32)
    lanes = min(128, rows)

    def col_copy(i):
        return pltpu.make_async_remote_copy(
            src_ref=cols.at[i], dst_ref=cols_in.at[spot], send_sem=col_send.at[i], recv_sem=col_recv.at[spot],
            device_id=chain_dev(i), device_id_type=MESH,
        )

    def col_arrival(i):
        return pltpu.make_async_remote_copy(
            src_ref=cols.at[i], dst_ref=cols_in.at[i], send_sem=col_send.at[i], recv_sem=col_recv.at[i],
            device_id=chain_dev(i), device_id_type=MESH,
        )

    def columns(d, carry):
        i = lax.rem(spot + d, chain)

        def one(u, carry):
            b = u // groups
            g = lax.rem(u, groups)
            acc = jnp.zeros((block, lanes), jnp.float32)
            for slot in range(2):
                where = (b * 2 + slot) * groups + g
                for r in range(rows // lanes):
                    w = ws[i, where, :, r * lanes:(r + 1) * lanes]
                    acc += es[i, b, slot, g, :, r * lanes:(r + 1) * lanes] * w
            summed = lax.dot_general(
                ones, acc, (((1,), (1,)), ((), ())), preferred_element_type=jnp.float32,
                precision=lax.Precision.HIGHEST,
            )
            cols[i, pl.ds(u, 1), :] = summed[0:1]
            return carry

        lax.fori_loop(0, requests * groups, one, 0)

        @pl.when(i != spot)
        def _():
            col_copy(i).start()

        return carry

    lax.fori_loop(1, chain + 1, columns, 0)

    def gather(d, acc):
        i = lax.rem(spot + d, chain)
        col_arrival(i).wait_recv()
        return acc + cols_in[i]

    result = lax.fori_loop(1, chain, gather, cols[spot])
    for b in range(requests):
        key_out[b] = result[b * groups:(b + 1) * groups]
        t = result[b * groups:b * groups + 1]
        for g in range(1, groups):
            t += result[b * groups + g:b * groups + g + 1]
        tok[b:b + 1, :] = t

    tok_copies = []
    for d in range(1, n_head):
        tok_copies.append(
            pltpu.make_async_remote_copy(
                src_ref=tok, dst_ref=tok_in.at[d], send_sem=tok_send.at[d], recv_sem=tok_recv.at[d],
                device_id=at(me, lax.rem(head + d, n_head)), device_id_type=MESH,
            )
        )
    for c in tok_copies:
        c.start()
    for c in tok_copies:
        c.wait_recv()
    tok_in[0] = tok[...]
    def head_sum(h, acc):
        return acc + tok_in[lax.rem(head - h + n_head, n_head)]

    tok_out[...] = lax.fori_loop(0, n_head, head_sum, jnp.zeros(tok.shape, jnp.float32))

    for c in tok_copies:
        c.wait_send()
    for d in range(1, chain):
        col_copy(lax.rem(spot + d, chain)).wait_send()
    for b in range(requests):
        query_copy(b).wait_send()

        def sent(i, carry):
            @pl.when((i <= spot) & (spot < chain - 1))
            def _():
                key_copy(i, b, True).wait_send()

            @pl.when((i >= spot) & (spot > 0))
            def _():
                key_copy(i, b, False).wait_send()

            return carry

        lax.fori_loop(0, chain, sent, 0)


def body(n_seq, n_head, queries, keys, lengths, starts):
    requests, tokens, width = queries.shape
    block = keys.shape[1]
    groups = keys.shape[2] // D
    heads = width // (groups * D)
    rows = heads * tokens
    chain = n_seq // 2
    units = requests * 2 * groups
    f32 = jnp.float32
    dma = pltpu.SemaphoreType.DMA
    any_spec = pl.BlockSpec(memory_space=pl.ANY)
    smem = pl.BlockSpec(memory_space=pltpu.SMEM)
    vmem = pl.BlockSpec(memory_space=pltpu.VMEM)
    return pl.pallas_call(
        functools.partial(kernel, n_seq, n_head),
        out_shape=(
            jax.ShapeDtypeStruct((requests, groups, block), f32),
            jax.ShapeDtypeStruct((requests, block), f32),
        ),
        in_specs=[smem, smem, any_spec, any_spec],
        out_specs=(vmem, vmem),
        scratch_shapes=[
            pltpu.VMEM((2, requests, groups, heads, tokens, D), queries.dtype),
            pltpu.VMEM((chain, requests, block, groups * D), keys.dtype),
            pltpu.VMEM((chain, requests, 2, groups, block, rows), f32),
            pltpu.VMEM((chain, units, rows), f32),
            pltpu.VMEM((chain, units, rows), f32),
            pltpu.VMEM((chain, units, 1, rows), f32),
            pltpu.VMEM((2, units, rows), f32),
            pltpu.VMEM((2, units, rows), f32),
            pltpu.VMEM((chain, requests * groups, block), f32),
            pltpu.VMEM((chain, requests * groups, block), f32),
            pltpu.VMEM((requests, block), f32),
            pltpu.VMEM((n_head, requests, block), f32),
            dma((requests,)), dma((requests,)), dma((requests,)), dma((requests,)),
            dma((chain, requests)), dma((chain, requests)), dma((chain, requests)),
            dma, dma, dma((chain,)), dma((chain,)), dma((n_head,)), dma((n_head,)),
        ],
        compiler_params=pltpu.CompilerParams(
            collective_id=0, has_side_effects=True, vmem_limit_bytes=60 * 1024 * 1024
        ),
    )(starts, lengths, queries, keys)


def solution(mesh):
    placed = (P(None, "seq", "head"), P(None, "seq", "head"), P(), P())
    return jax.shard_map(
        functools.partial(body, mesh.shape["seq"], mesh.shape["head"]),
        mesh=mesh,
        in_specs=placed,
        out_specs=(P(None, "head", "seq"), P(None, "seq")),
        check_vma=False,
    )
```

```python
import functools

import jax
import jax.numpy as jnp
from jax import lax
from jax.experimental import pallas as pl
from jax.experimental.pallas import tpu as pltpu
from jax.sharding import PartitionSpec as P

KVH = 8
D = 128
QLEN = 512
MASK_FILL = -1e30
MASK_FLOOR = -5e29
LOG2E = 1.4426950408889634
MESH = pl.DeviceIdType.MESH


def kernel(
    n_seq, n_head, starts_ref, lengths_ref, q_hbm, k_hbm, key_out, tok_out,
    qs, ks, es, ms, ls, ws, stat, stat_in, cols, cols_in, tok, tok_in,
    q_sem, k_sem, q_send, q_recv, up_send, down_send, k_recv,
    stat_send, stat_recv, col_send, col_recv, tok_send, tok_recv,
):
    requests, tokens, width = q_hbm.shape
    block = k_hbm.shape[1]
    groups = k_hbm.shape[2] // D
    heads = width // (groups * D)
    rows = heads * tokens
    items = requests * groups
    chain = n_seq // 2
    last = chain - 1
    tile = min(256, rows)
    lanes = min(128, rows)
    scale = (D ** -0.5) * LOG2E
    me = lax.axis_index("seq")
    head = lax.axis_index("head")
    pair = lax.rem(me, 2)
    spot = me // 2
    own, other = pair, 1 - pair

    def at(seq, hd=None):
        return {"seq": seq, "head": head if hd is None else hd}

    def chain_dev(i, hd=None):
        return at(i * 2 + pair, hd)

    def head_at(d):
        return lax.rem(head + d, n_head)

    peer = at(me + 1 - 2 * pair)

    def key_load(u):
        b, g = divmod(u, groups)
        return pltpu.make_async_copy(k_hbm.at[b, :, pl.ds(g * D, D)], ks.at[spot, u], k_sem.at[u])

    for u in range(items):
        key_load(u).start()
    for u in range(items):
        b, g = divmod(u, groups)
        for h in range(heads):
            pltpu.make_async_copy(
                q_hbm.at[b, :, pl.ds((g * heads + h) * D, D)], qs.at[pair, u, h], q_sem.at[u]
            ).start()

    barrier = pltpu.get_barrier_semaphore()

    def greet(device):
        pl.semaphore_signal(barrier, inc=1, device_id=device, device_id_type=MESH)

    @pl.when(spot > 0)
    def _():
        greet(chain_dev(spot - 1))

    @pl.when(spot < last)
    def _():
        greet(chain_dev(spot + 1))

    greet(peer)
    for d in range(1, n_head):
        greet(at(me, head_at(d)))
    inner = jnp.where(spot > 0, 1, 0) + jnp.where(spot < last, 1, 0)
    pl.semaphore_wait(barrier, inner + n_head)

    def key_copy(i, u, upward):
        sems = up_send if upward else down_send
        return pltpu.make_async_remote_copy(
            src_ref=ks.at[i, u], dst_ref=ks.at[i, u], send_sem=sems.at[i, u], recv_sem=k_recv.at[i, u],
            device_id=chain_dev(spot + 1 if upward else spot - 1), device_id_type=MESH,
        )

    def send_key(i, u, upward):
        @pl.when((spot < last) if upward else (spot > 0))
        def _():
            key_copy(i, u, upward).start()

    def query_copy(u):
        return pltpu.make_async_remote_copy(
            src_ref=qs.at[pair, u], dst_ref=qs.at[pair, u], send_sem=q_send.at[u], recv_sem=q_recv.at[u],
            device_id=peer, device_id_type=MESH,
        )

    for u in range(items):
        key_load(u).wait()
        send_key(spot, u, True)
        send_key(spot, u, False)
    for u in range(items):
        pltpu.make_async_copy(qs.at[pair, u], qs.at[pair, u], q_sem.at[u]).wait()
        query_copy(u).start()

    lane_token = lax.rem(lax.broadcasted_iota(jnp.int32, (1, tile), 1), tokens)
    key_row = lax.broadcasted_iota(jnp.int32, (block, 1), 0)

    def work(i, u, first, count):
        start = starts_ref[u // groups]
        length = lengths_ref[u // groups]
        keypos = (i * 2 + pair) * block + key_row
        keypos = jnp.where(keypos >= start, keypos, 2 ** 30)
        k = ks[i, u]

        def step(v, carry):
            slot = lax.rem(first + v, 2)
            q = qs[slot, u].reshape(rows, D)
            pos = length - QLEN + (spot * 2 + slot) * tokens + lane_token
            for r in range(rows // tile):
                part = slice(r * tile, (r + 1) * tile)
                s = lax.dot_general(
                    k, q[part], (((1,), (1,)), ((), ())), preferred_element_type=jnp.float32
                )
                s = jnp.where(keypos <= pos, s, MASK_FILL)
                top = jnp.maximum(jnp.max(s, axis=0, keepdims=True), MASK_FLOOR)
                e = jnp.exp2((s - top) * scale)
                es[i, u, slot, :, part] = e
                ms[i, u, pl.ds(slot, 1), part] = top
                ls[i, u, pl.ds(slot, 1), part] = jnp.sum(e, axis=0, keepdims=True)
            return carry

        lax.fori_loop(0, count, step, 0)

    def arrive(s, u):
        @pl.when(spot - s >= 0)
        def _():
            key_copy(spot - s, u, True).wait_recv()
            send_key(spot - s, u, True)

        @pl.when(spot + s < chain)
        def _():
            key_copy(spot + s, u, False).wait_recv()
            send_key(spot + s, u, False)

    def sides(s, u, count):
        def side(v, carry):
            i = spot - s + v * 2 * s

            @pl.when((i >= 0) & (i < chain))
            def _():
                work(i, u, own, count)

            return carry

        lax.fori_loop(0, 2, side, 0)

    def catch_up(u, reach):
        query_copy(u).wait_recv()

        def one(i, carry):
            work(i, u, other, 1)
            return carry

        lax.fori_loop(jnp.maximum(spot - reach, 0), jnp.minimum(spot + reach, last) + 1, one, 0)

    def stat_copy(u):
        return pltpu.make_async_remote_copy(
            src_ref=stat.at[u], dst_ref=stat_in.at[u], send_sem=stat_send.at[u], recv_sem=stat_recv.at[u],
            device_id=peer, device_id_type=MESH,
        )

    def summarize(u):
        top = ms[0, u]
        for i in range(1, chain):
            top = jnp.maximum(top, ms[i, u])
        total = ls[0, u] * jnp.exp2((ms[0, u] - top) * scale)
        for i in range(1, chain):
            total += ls[i, u] * jnp.exp2((ms[i, u] - top) * scale)
        stat[u, 0] = top
        stat[u, 1] = total
        stat_copy(u).start()

    def col_copy(i, b):
        return pltpu.make_async_remote_copy(
            src_ref=cols.at[i, b], dst_ref=cols_in.at[spot, b], send_sem=col_send.at[i, b],
            recv_sem=col_recv.at[spot, b], device_id=chain_dev(i), device_id_type=MESH,
        )

    def tok_copy(i, d, b):
        return pltpu.make_async_remote_copy(
            src_ref=tok.at[i, b], dst_ref=tok_in.at[spot, d, b], send_sem=tok_send.at[i, d, b],
            recv_sem=tok_recv.at[spot, d, b], device_id=chain_dev(i, head_at(d)), device_id_type=MESH,
        )

    ones = jnp.ones((8, lanes), jnp.float32)

    def finish(u):
        b, g = divmod(u, groups)
        stat_copy(u).wait_recv()
        full_top = jnp.maximum(stat[u, 0], stat_in[u, 0])
        full = stat[u, 1] * jnp.exp2((stat[u, 0] - full_top) * scale) + stat_in[u, 1] * jnp.exp2(
            (stat_in[u, 0] - full_top) * scale
        )
        inverse = 1.0 / full
        for i in range(chain):
            weight = jnp.exp2((ms[i, u] - full_top) * scale) * inverse
            for slot in range(2):
                ws[i, slot] = weight[slot:slot + 1]

        def columns(d, carry):
            i = lax.rem(spot + d, chain)
            acc = jnp.zeros((block, lanes), jnp.float32)
            for slot in range(2):
                for r in range(rows // lanes):
                    part = slice(r * lanes, (r + 1) * lanes)
                    acc += es[i, u, slot, :, part] * ws[i, slot, :, part]
            summed = lax.dot_general(
                ones, acc, (((1,), (1,)), ((), ())), preferred_element_type=jnp.float32,
                precision=lax.Precision.HIGHEST,
            )[0:1]
            cols[i, b, g:g + 1, :] = summed
            if g == groups - 1:
                for other_g in range(groups - 1):
                    summed = cols[i, b, other_g:other_g + 1, :] + summed
                tok[i, b] = summed

                @pl.when(i != spot)
                def _():
                    col_copy(i, b).start()

                for h in range(1, n_head):
                    tok_copy(i, h, b).start()
            return carry

        lax.fori_loop(1, chain + 1, columns, 0)

    def closing(u):
        summarize(u)
        if u > 0:
            finish(u - 1)

    def stage(s, caught, final):
        for u in range(items):
            arrive(s, u)
            if caught:
                catch_up(u, s - 1)
            sides(s, u, 2 if s >= 2 or caught else 1)
            if final:
                closing(u)

    for u in range(items):
        work(spot, u, own, 1)
    if last == 0:
        for u in range(items):
            catch_up(u, 0)
            closing(u)
    if last >= 1:
        stage(1, last == 1, last == 1)
    if last >= 2:
        stage(2, True, last == 2)
    if last >= 3:
        def middle(s, carry):
            for u in range(items):
                arrive(s, u)
                sides(s, u, 2)
            return carry

        lax.fori_loop(3, last, middle, 0)
        stage(last, False, True)
    finish(items - 1)

    for b in range(requests):
        cols_in[spot, b] = cols[spot, b]

        def landed(i, carry):
            @pl.when(i != spot)
            def _():
                col_arrival = pltpu.make_async_remote_copy(
                    src_ref=cols.at[i, b], dst_ref=cols_in.at[i, b], send_sem=col_send.at[i, b],
                    recv_sem=col_recv.at[i, b], device_id=chain_dev(i), device_id_type=MESH,
                )
                col_arrival.wait_recv()

            for d in range(1, n_head):
                tok_arrival = pltpu.make_async_remote_copy(
                    src_ref=tok.at[i, b], dst_ref=tok_in.at[i, d, b], send_sem=tok_send.at[i, d, b],
                    recv_sem=tok_recv.at[i, d, b], device_id=chain_dev(i, head_at(d)), device_id_type=MESH,
                )
                tok_arrival.wait_recv()
            return carry

        lax.fori_loop(0, chain, landed, 0)

        def gather(i, acc):
            return acc + cols_in[i, b]

        key_out[b] = lax.fori_loop(1, chain, gather, cols_in[0, b])
        for i in range(chain):
            part = cols_in[i, b, groups - 1:groups, :]
            for g in range(groups - 1):
                part = cols_in[i, b, g:g + 1, :] + part
            tok_in[i, 0, b] = part

        def head_sum(h, acc):
            d = lax.rem(head - h + n_head, n_head)
            for i in range(chain):
                acc = acc + tok_in[i, d, b]
            return acc

        tok_out[b:b + 1, :] = lax.fori_loop(0, n_head, head_sum, jnp.zeros((1, block), jnp.float32))

    def sent(i, carry):
        for b in range(requests):
            @pl.when(i != spot)
            def _():
                col_copy(i, b).wait_send()

            for d in range(1, n_head):
                tok_copy(i, d, b).wait_send()
        for u in range(items):
            @pl.when((i <= spot) & (spot < last))
            def _():
                key_copy(i, u, True).wait_send()

            @pl.when((i >= spot) & (spot > 0))
            def _():
                key_copy(i, u, False).wait_send()

        return carry

    lax.fori_loop(0, chain, sent, 0)
    for u in range(items):
        query_copy(u).wait_send()
        stat_copy(u).wait_send()


def body(n_seq, n_head, queries, keys, lengths, starts):
    requests, tokens, width = queries.shape
    block = keys.shape[1]
    groups = keys.shape[2] // D
    heads = width // (groups * D)
    rows = heads * tokens
    chain = n_seq // 2
    items = requests * groups
    f32 = jnp.float32
    dma = pltpu.SemaphoreType.DMA
    any_spec = pl.BlockSpec(memory_space=pl.ANY)
    smem = pl.BlockSpec(memory_space=pltpu.SMEM)
    vmem = pl.BlockSpec(memory_space=pltpu.VMEM)
    return pl.pallas_call(
        functools.partial(kernel, n_seq, n_head),
        out_shape=(
            jax.ShapeDtypeStruct((requests, groups, block), f32),
            jax.ShapeDtypeStruct((requests, block), f32),
        ),
        in_specs=[smem, smem, any_spec, any_spec],
        out_specs=(vmem, vmem),
        scratch_shapes=[
            pltpu.VMEM((2, items, heads, tokens, D), queries.dtype),
            pltpu.VMEM((chain, items, block, D), keys.dtype),
            pltpu.VMEM((chain, items, 2, block, rows), f32),
            pltpu.VMEM((chain, items, 2, rows), f32),
            pltpu.VMEM((chain, items, 2, rows), f32),
            pltpu.VMEM((chain, 2, 1, rows), f32),
            pltpu.VMEM((items, 2, 2, rows), f32),
            pltpu.VMEM((items, 2, 2, rows), f32),
            pltpu.VMEM((chain, requests, groups, block), f32),
            pltpu.VMEM((chain, requests, groups, block), f32),
            pltpu.VMEM((chain, requests, 1, block), f32),
            pltpu.VMEM((chain, n_head, requests, 1, block), f32),
            dma((items,)), dma((items,)), dma((items,)), dma((items,)),
            dma((chain, items)), dma((chain, items)), dma((chain, items)),
            dma((items,)), dma((items,)), dma((chain, requests)), dma((chain, requests)),
            dma((chain, n_head, requests)), dma((chain, n_head, requests)),
        ],
        compiler_params=pltpu.CompilerParams(
            collective_id=0, has_side_effects=True, vmem_limit_bytes=60 * 1024 * 1024
        ),
    )(starts, lengths, queries, keys)


def solution(mesh):
    placed = (P(None, "seq", "head"), P(None, "seq", "head"), P(), P())
    return jax.shard_map(
        functools.partial(body, mesh.shape["seq"], mesh.shape["head"]),
        mesh=mesh,
        in_specs=placed,
        out_specs=(P(None, "head", "seq"), P(None, "seq")),
        check_vma=False,
    )
```

```python
import functools

import jax
import jax.numpy as jnp
from jax import lax
from jax.experimental import pallas as pl
from jax.experimental.pallas import tpu as pltpu
from jax.sharding import PartitionSpec as P

KVH = 8
D = 128
QLEN = 512
MASK_FILL = -1e30
MASK_FLOOR = -5e29
LOG2E = 1.4426950408889634
MESH = pl.DeviceIdType.MESH


def kernel(
    n_seq, n_head, starts_ref, lengths_ref, q_hbm, k_hbm, packed_out,
    qs, ks, es, ms, ls, ws, stat, stat_in, cols, cols_in, tok, tok_in,
    q_sem, k_sem, q_send, q_recv, up_send, down_send, k_recv,
    stat_send, stat_recv, col_send, col_recv, tok_send, tok_recv,
):
    requests, tokens, width = q_hbm.shape
    block = k_hbm.shape[1]
    groups = k_hbm.shape[2] // D
    heads = width // (groups * D)
    rows = heads * tokens
    items = requests * groups
    chain = n_seq // 2
    last = chain - 1
    tile = min(256, rows)
    lanes = min(128, rows)
    scale = (D ** -0.5) * LOG2E
    me = lax.axis_index("seq")
    head = lax.axis_index("head")
    pair = lax.rem(me, 2)
    spot = me // 2
    own, other = pair, 1 - pair

    def at(seq, hd=None):
        return {"seq": seq, "head": head if hd is None else hd}

    def chain_dev(i, hd=None):
        return at(i * 2 + pair, hd)

    def head_at(d):
        return lax.rem(head + d, n_head)

    peer = at(me + 1 - 2 * pair)

    def key_load(u):
        b, g = divmod(u, groups)
        return pltpu.make_async_copy(k_hbm.at[b, :, pl.ds(g * D, D)], ks.at[spot, u], k_sem.at[u])

    for u in range(items):
        key_load(u).start()
    for u in range(items):
        b, g = divmod(u, groups)
        for h in range(heads):
            pltpu.make_async_copy(
                q_hbm.at[b, :, pl.ds((g * heads + h) * D, D)], qs.at[pair, u, h], q_sem.at[u]
            ).start()

    barrier = pltpu.get_barrier_semaphore()

    def greet(device):
        pl.semaphore_signal(barrier, inc=1, device_id=device, device_id_type=MESH)

    @pl.when(spot > 0)
    def _():
        greet(chain_dev(spot - 1))

    @pl.when(spot < last)
    def _():
        greet(chain_dev(spot + 1))

    greet(peer)
    for d in range(1, n_head):
        greet(at(me, head_at(d)))
    inner = jnp.where(spot > 0, 1, 0) + jnp.where(spot < last, 1, 0)
    pl.semaphore_wait(barrier, inner + n_head)

    def key_copy(i, u, upward):
        sems = up_send if upward else down_send
        return pltpu.make_async_remote_copy(
            src_ref=ks.at[i, u], dst_ref=ks.at[i, u], send_sem=sems.at[i, u], recv_sem=k_recv.at[i, u],
            device_id=chain_dev(spot + 1 if upward else spot - 1), device_id_type=MESH,
        )

    def send_key(i, u, upward):
        @pl.when((spot < last) if upward else (spot > 0))
        def _():
            key_copy(i, u, upward).start()

    def query_copy(u):
        return pltpu.make_async_remote_copy(
            src_ref=qs.at[pair, u], dst_ref=qs.at[pair, u], send_sem=q_send.at[u], recv_sem=q_recv.at[u],
            device_id=peer, device_id_type=MESH,
        )

    for u in range(items):
        key_load(u).wait()
        send_key(spot, u, True)
        send_key(spot, u, False)
    for u in range(items):
        pltpu.make_async_copy(qs.at[pair, u], qs.at[pair, u], q_sem.at[u]).wait()
        query_copy(u).start()

    lane_token = lax.rem(lax.broadcasted_iota(jnp.int32, (1, tile), 1), tokens)
    key_row = lax.broadcasted_iota(jnp.int32, (block, 1), 0)

    def work(i, u, first, count):
        start = starts_ref[u // groups]
        length = lengths_ref[u // groups]
        keypos = (i * 2 + pair) * block + key_row
        keypos = jnp.where(keypos >= start, keypos, 2 ** 30)
        k = ks[i, u]

        def step(v, carry):
            slot = lax.rem(first + v, 2)
            q = qs[slot, u].reshape(rows, D)
            pos = length - QLEN + (spot * 2 + slot) * tokens + lane_token
            for r in range(rows // tile):
                part = slice(r * tile, (r + 1) * tile)
                s = lax.dot_general(
                    k, q[part], (((1,), (1,)), ((), ())), preferred_element_type=jnp.float32
                )
                s = jnp.where(keypos <= pos, s, MASK_FILL)
                top = jnp.maximum(jnp.max(s, axis=0, keepdims=True), MASK_FLOOR)
                e = jnp.exp2((s - top) * scale)
                es[i, u, slot, :, part] = e
                ms[i, u, pl.ds(slot, 1), part] = top
                ls[i, u, pl.ds(slot, 1), part] = jnp.sum(e, axis=0, keepdims=True)
            return carry

        lax.fori_loop(0, count, step, 0)

    def arrive(s, u):
        @pl.when(spot - s >= 0)
        def _():
            key_copy(spot - s, u, True).wait_recv()
            send_key(spot - s, u, True)

        @pl.when(spot + s < chain)
        def _():
            key_copy(spot + s, u, False).wait_recv()
            send_key(spot + s, u, False)

    def sides(s, u, count):
        def side(v, carry):
            i = spot - s + v * 2 * s

            @pl.when((i >= 0) & (i < chain))
            def _():
                work(i, u, own, count)

            return carry

        lax.fori_loop(0, 2, side, 0)

    def catch_up(u, reach):
        query_copy(u).wait_recv()

        def one(i, carry):
            work(i, u, other, 1)
            return carry

        lax.fori_loop(jnp.maximum(spot - reach, 0), jnp.minimum(spot + reach, last) + 1, one, 0)

    def stat_copy(u):
        return pltpu.make_async_remote_copy(
            src_ref=stat.at[u], dst_ref=stat_in.at[u], send_sem=stat_send.at[u], recv_sem=stat_recv.at[u],
            device_id=peer, device_id_type=MESH,
        )

    def summarize(u):
        top = ms[0, u]
        for i in range(1, chain):
            top = jnp.maximum(top, ms[i, u])
        total = ls[0, u] * jnp.exp2((ms[0, u] - top) * scale)
        for i in range(1, chain):
            total += ls[i, u] * jnp.exp2((ms[i, u] - top) * scale)
        stat[u, 0] = top
        stat[u, 1] = total
        stat_copy(u).start()

    def col_copy(i, b):
        return pltpu.make_async_remote_copy(
            src_ref=cols.at[i, b], dst_ref=cols_in.at[spot, b], send_sem=col_send.at[i, b],
            recv_sem=col_recv.at[spot, b], device_id=chain_dev(i), device_id_type=MESH,
        )

    def tok_copy(i, d, b):
        return pltpu.make_async_remote_copy(
            src_ref=tok.at[i, b], dst_ref=tok_in.at[spot, d, b], send_sem=tok_send.at[i, d, b],
            recv_sem=tok_recv.at[spot, d, b], device_id=chain_dev(i, head_at(d)), device_id_type=MESH,
        )

    ones = jnp.ones((8, lanes), jnp.float32)

    def finish(u):
        b, g = divmod(u, groups)
        stat_copy(u).wait_recv()
        full_top = jnp.maximum(stat[u, 0], stat_in[u, 0])
        full = stat[u, 1] * jnp.exp2((stat[u, 0] - full_top) * scale) + stat_in[u, 1] * jnp.exp2(
            (stat_in[u, 0] - full_top) * scale
        )
        inverse = 1.0 / full
        for i in range(chain):
            weight = jnp.exp2((ms[i, u] - full_top) * scale) * inverse
            for slot in range(2):
                ws[i, slot] = weight[slot:slot + 1]

        def columns(d, carry):
            i = jnp.where(2 * spot < chain, last - d, d)
            acc = jnp.zeros((block, lanes), jnp.float32)
            for slot in range(2):
                for r in range(rows // lanes):
                    part = slice(r * lanes, (r + 1) * lanes)
                    acc += es[i, u, slot, :, part] * ws[i, slot, :, part]
            summed = lax.dot_general(
                ones, acc, (((1,), (1,)), ((), ())), preferred_element_type=jnp.float32,
                precision=lax.Precision.HIGHEST,
            )[0:1]
            cols[i, b, g:g + 1, :] = summed
            if g == groups - 1:
                for other_g in range(groups - 1):
                    summed = cols[i, b, other_g:other_g + 1, :] + summed
                tok[i, b] = summed

                @pl.when(i != spot)
                def _():
                    col_copy(i, b).start()

                for h in range(1, n_head):
                    tok_copy(i, h, b).start()
            return carry

        lax.fori_loop(0, chain, columns, 0)

    def closing(u):
        summarize(u)
        if u > 0:
            finish(u - 1)

    def stage(s, caught, final):
        for u in range(items):
            arrive(s, u)
            if caught:
                catch_up(u, s - 1)
            sides(s, u, 2 if s >= 2 or caught else 1)
            if final:
                closing(u)

    for u in range(items):
        work(spot, u, own, 1)
    if last == 0:
        for u in range(items):
            catch_up(u, 0)
            closing(u)
    if last >= 1:
        stage(1, last == 1, last == 1)
    if last >= 2:
        stage(2, True, last == 2)
    if last >= 3:
        def middle(s, carry):
            for u in range(items):
                arrive(s, u)
                sides(s, u, 2)
            return carry

        lax.fori_loop(3, last, middle, 0)
        stage(last, False, True)
    finish(items - 1)

    for b in range(requests):
        cols_in[spot, b] = cols[spot, b]

        def landed(i, carry):
            @pl.when(i != spot)
            def _():
                col_arrival = pltpu.make_async_remote_copy(
                    src_ref=cols.at[i, b], dst_ref=cols_in.at[i, b], send_sem=col_send.at[i, b],
                    recv_sem=col_recv.at[i, b], device_id=chain_dev(i), device_id_type=MESH,
                )
                col_arrival.wait_recv()

            for d in range(1, n_head):
                tok_arrival = pltpu.make_async_remote_copy(
                    src_ref=tok.at[i, b], dst_ref=tok_in.at[i, d, b], send_sem=tok_send.at[i, d, b],
                    recv_sem=tok_recv.at[i, d, b], device_id=chain_dev(i, head_at(d)), device_id_type=MESH,
                )
                tok_arrival.wait_recv()
            return carry

        lax.fori_loop(0, chain, landed, 0)

        def gather(i, acc):
            return acc + cols_in[i, b]

        packed_out[b * groups:(b + 1) * groups, :] = lax.fori_loop(1, chain, gather, cols_in[0, b])
        for i in range(chain):
            part = cols_in[i, b, groups - 1:groups, :]
            for g in range(groups - 1):
                part = cols_in[i, b, g:g + 1, :] + part
            tok_in[i, 0, b] = part

        def head_sum(h, acc):
            d = lax.rem(head - h + n_head, n_head)
            for i in range(chain):
                acc = acc + tok_in[i, d, b]
            return acc

        packed_out[items + b:items + b + 1, :] = lax.fori_loop(0, n_head, head_sum, jnp.zeros((1, block), jnp.float32))

    def sent(i, carry):
        for b in range(requests):
            @pl.when(i != spot)
            def _():
                col_copy(i, b).wait_send()

            for d in range(1, n_head):
                tok_copy(i, d, b).wait_send()
        for u in range(items):
            @pl.when((i <= spot) & (spot < last))
            def _():
                key_copy(i, u, True).wait_send()

            @pl.when((i >= spot) & (spot > 0))
            def _():
                key_copy(i, u, False).wait_send()

        return carry

    lax.fori_loop(0, chain, sent, 0)
    for u in range(items):
        query_copy(u).wait_send()
        stat_copy(u).wait_send()


def body(n_seq, n_head, queries, keys, lengths, starts):
    requests, tokens, width = queries.shape
    block = keys.shape[1]
    groups = keys.shape[2] // D
    heads = width // (groups * D)
    rows = heads * tokens
    chain = n_seq // 2
    items = requests * groups
    f32 = jnp.float32
    dma = pltpu.SemaphoreType.DMA
    any_spec = pl.BlockSpec(memory_space=pl.ANY)
    smem = pl.BlockSpec(memory_space=pltpu.SMEM)
    vmem = pl.BlockSpec(memory_space=pltpu.VMEM)
    packed = pl.pallas_call(
        functools.partial(kernel, n_seq, n_head),
        out_shape=jax.ShapeDtypeStruct((items + requests, block), f32),
        in_specs=[smem, smem, any_spec, any_spec],
        out_specs=vmem,
        scratch_shapes=[
            pltpu.VMEM((2, items, heads, tokens, D), queries.dtype),
            pltpu.VMEM((chain, items, block, D), keys.dtype),
            pltpu.VMEM((chain, items, 2, block, rows), f32),
            pltpu.VMEM((chain, items, 2, rows), f32),
            pltpu.VMEM((chain, items, 2, rows), f32),
            pltpu.VMEM((chain, 2, 1, rows), f32),
            pltpu.VMEM((items, 2, 2, rows), f32),
            pltpu.VMEM((items, 2, 2, rows), f32),
            pltpu.VMEM((chain, requests, groups, block), f32),
            pltpu.VMEM((chain, requests, groups, block), f32),
            pltpu.VMEM((chain, requests, 1, block), f32),
            pltpu.VMEM((chain, n_head, requests, 1, block), f32),
            dma((items,)), dma((items,)), dma((items,)), dma((items,)),
            dma((chain, items)), dma((chain, items)), dma((chain, items)),
            dma((items,)), dma((items,)), dma((chain, requests)), dma((chain, requests)),
            dma((chain, n_head, requests)), dma((chain, n_head, requests)),
        ],
        compiler_params=pltpu.CompilerParams(
            collective_id=0, has_side_effects=True, vmem_limit_bytes=60 * 1024 * 1024
        ),
    )(starts, lengths, queries, keys)

    def unpack(packed_ref, key_ref, tok_ref):
        for b in range(requests):
            key_ref[b] = packed_ref[b * groups:(b + 1) * groups]
        tok_ref[...] = packed_ref[items:]

    return pl.pallas_call(
        unpack,
        out_shape=(
            jax.ShapeDtypeStruct((requests, groups, block), f32),
            jax.ShapeDtypeStruct((requests, block), f32),
        ),
    )(packed)


def solution(mesh):
    placed = (P(None, "seq", "head"), P(None, "seq", "head"), P(), P())
    return jax.shard_map(
        functools.partial(body, mesh.shape["seq"], mesh.shape["head"]),
        mesh=mesh,
        in_specs=placed,
        out_specs=(P(None, "head", "seq"), P(None, "seq")),
        check_vma=False,
    )
```
